32 devices in a mesh: gx: 8 (over y, x, core), gy: 4 (over z).
Axes of the slice: x: 2, y: 2, z: 4, core: 2. Of those that a mesh axis runs over, the one named last changes fastest.
Arguments:
- snapshots: bfloat16 [2, 1, 256, 256, 512], P(None, None, 'gx', 'gy'), may hold values from -12 to 12
- start: float32 [1, 32, 256, 256], P(None, None, 'gx', 'gy'), may hold values from -6 to 6
Outputs:
- basis_field: float32 [1, 32, 256, 256], P(None, None, 'gx', 'gy')
- phi: float32 [1, 2, 32, 32], replicated
The draws below stay inside these ranges and needn't reach their ends.
All inputs are finite; a program needn't handle non-finite values.
Results may differ from the reference program's by a relative error of at most 0.0005.
Values may be sent and summed in bfloat16 or wider, within the bound.
A program may use at most 64 MiB of HBM per device.

```python
import math
import jax
import jax.numpy as jnp
from jax import lax

NR = 256
NC = 256
K = 32
S = 1024
ITERS = 4
F = 1
S0 = 512


def draw_snapshots(key, part):
    keys = jax.random.split(key, 7)
    row_angle = jax.random.uniform(keys[0], (F, K), jnp.float32, -2.0, 2.0)
    col_angle = jax.random.uniform(keys[1], (F, K), jnp.float32, -2.0, 2.0)
    log_power = jax.random.uniform(keys[2], (F, K), jnp.float32, math.log(2.0 / S), math.log(16.0 / S))
    amplitude = jnp.sqrt(jnp.exp(log_power) / 2.0)
    row_place = jnp.arange(NR, dtype=jnp.float32) - (NR - 1) / 2.0
    col_place = jnp.arange(NC, dtype=jnp.float32) - (NC - 1) / 2.0
    phase = row_angle[:, :, None, None] * row_place[None, None, :, None] + col_angle[:, :, None, None] * col_place[None, None, None, :]
    phase = phase.reshape(F, K, NR * NC)
    cosine = jnp.cos(phase)
    sine = jnp.sin(phase)
    signal_real = jax.random.normal(keys[3], (F, K, S0), jnp.float32) * amplitude[:, :, None]
    signal_imag = jax.random.normal(keys[4], (F, K, S0), jnp.float32) * amplitude[:, :, None]
    wave_real = jnp.einsum('fkm,fks->fms', cosine, signal_real) - jnp.einsum('fkm,fks->fms', sine, signal_imag)
    wave_imag = jnp.einsum('fkm,fks->fms', cosine, signal_imag) + jnp.einsum('fkm,fks->fms', sine, signal_real)
    noise_real = jax.random.normal(keys[5], (F, NR * NC, S0), jnp.float32)
    noise_imag = jax.random.normal(keys[6], (F, NR * NC, S0), jnp.float32)
    stacked = jnp.stack([wave_real + noise_real, wave_imag + noise_imag])
    stacked = jnp.clip(stacked, -12.0, 12.0).reshape(2, F, NR, NC, S0)
    return stacked.astype(jnp.bfloat16)


def levels(key, dims, cuts, low, high):
    def one(dim, shards_of):
        heights = jax.random.uniform(jax.random.fold_in(jax.random.fold_in(key, 6), dim), (shards_of,), jnp.float32, low / len(cuts), high / len(cuts))
        return jnp.repeat(jnp.exp(heights), dims[dim] // shards_of).reshape((-1,) + (1,) * (len(dims) - dim - 1))

    gain = one(*cuts[0])
    for cut in cuts[1:]:
        gain = gain * one(*cut)
    return gain


def normal_values(own_key, dims, deviation, most, shards=(), kind=jnp.bfloat16):
    array = deviation * jax.random.normal(own_key, dims, jnp.float32)
    if shards:
        array = array * levels(own_key, dims, shards, -0.22, 0.18)
    return jnp.clip(array, -most, most).astype(kind)


def setup_inputs(seed: int = 0) -> dict:
    splits = jax.random.split(jax.random.key(seed), 3)
    return {
        "snapshots": draw_snapshots(jax.random.fold_in(splits[2], 71), 0),
        "start": normal_values(splits[1], (F, K, NR, NC), 1.0, 6.0, ((2, 8), (3, 4)), jnp.float32),
    }


precise = lax.Precision.HIGHEST

def inverse_lower(matrix):
    factor = jnp.linalg.cholesky(matrix)
    identity = jnp.broadcast_to(jnp.eye(matrix.shape[-1], dtype=matrix.dtype), matrix.shape)
    inverse = lax.linalg.triangular_solve(factor, identity, left_side=True, lower=True)
    return inverse

def solve_shift(left_matrix, right_matrix):
    inverse = inverse_lower(left_matrix)
    inner = jnp.dot(inverse, right_matrix, precision=precise)
    return jnp.dot(inverse.T, inner, precision=precise)

def transform_frame(frame):
    direct = frame.astype(jnp.float32)
    mirror = direct[:, ::-1, ::-1, :]
    upper_rows = (jnp.arange(NR) < NR // 2)[:, None, None]
    first = jnp.where(upper_rows, direct[0] + mirror[0], direct[1] - mirror[1])
    second = jnp.where(upper_rows, -(direct[1] + mirror[1]), direct[0] - mirror[0])
    return jnp.concatenate([first, second], axis=-1).reshape(NR * NC, 2 * S0)

def pair_grams(plus_terms, minus_terms):
    left_matrix = jnp.einsum('kab,jab->kj', plus_terms, plus_terms, precision=precise)
    right_matrix = jnp.einsum('kab,jab->kj', plus_terms, minus_terms, precision=precise)
    return (left_matrix, right_matrix)

def one_frame(frame, start_frame):
    data = transform_frame(frame)
    basis = start_frame.reshape(K, NR * NC)
    for step_index in range(ITERS):
        side = jnp.dot(basis, data, precision=precise)
        grown = jnp.dot(side, data.T, precision=precise)
        gram = jnp.dot(grown, grown.T, precision=precise)
        inverse = inverse_lower(gram)
        basis = jnp.dot(inverse, grown, precision=precise)
    field = basis.reshape(K, NR, NC)
    row_lhs, row_rhs = pair_grams(field[:, 1:] + field[:, :-1], field[:, 1:] - field[:, :-1])
    col_lhs, col_rhs = pair_grams(field[:, :, 1:] + field[:, :, :-1], field[:, :, 1:] - field[:, :, :-1])
    phi_frame = jnp.stack([solve_shift(row_lhs, row_rhs), solve_shift(col_lhs, col_rhs)])
    return (field, phi_frame)

def reference(snapshots, start):
    fields = []
    phis = []
    for frame_index in range(F):
        field, phi_frame = one_frame(snapshots[:, frame_index], start[frame_index])
        fields.append(field)
        phis.append(phi_frame)
    return (jnp.stack(fields), jnp.stack(phis))
```

```python
import functools

import jax
import jax.numpy as jnp
from jax import lax
from jax.experimental import pallas as pl
from jax.experimental.pallas import tpu as pltpu
from jax.sharding import PartitionSpec as P

ITERS = 4
TILE = (8, 128)
MESH = pl.DeviceIdType.MESH

precise = lax.Precision.HIGHEST


def position():
    across = lax.axis_size("gy")
    return lax.axis_index("gx") * across + lax.axis_index("gy")


def device_of(index):
    across = lax.axis_size("gy")
    return (lax.div(index, across), lax.rem(index, across))


def device_count():
    return lax.axis_size("gx") * lax.axis_size("gy")


def enter():
    n = device_count()
    me = position()
    barrier = pltpu.get_barrier_semaphore()

    def greet(k, carry):
        pl.semaphore_signal(
            barrier, inc=1, device_id=device_of(lax.rem(me + k, n)), device_id_type=MESH
        )
        return carry

    lax.fori_loop(1, n, greet, 0)
    pl.semaphore_wait(barrier, n - 1)


def all_reduce(own, landed, total, gathered, send_a, recv_a, send_b, recv_b):
    n = device_count()
    me = position()
    tiles = own.shape[0]

    def scatter(k):
        owner = lax.rem(me + k, n)
        return owner, pltpu.make_async_remote_copy(
            src_ref=own.at[lax.rem(owner, tiles)],
            dst_ref=landed.at[k],
            send_sem=send_a.at[k],
            recv_sem=recv_a.at[k],
            device_id=device_of(owner),
            device_id_type=MESH,
        )

    def spread(k):
        return pltpu.make_async_remote_copy(
            src_ref=total,
            dst_ref=gathered.at[lax.rem(me, tiles)],
            send_sem=send_b.at[k],
            recv_sem=recv_b.at[k],
            device_id=device_of(lax.rem(me + k, n)),
            device_id_type=MESH,
        )

    def scatter_start(k, carry):
        owner, copy = scatter(k)
        if n == tiles:
            copy.start()
        else:
            pl.when(owner < tiles)(lambda: copy.start())
        return carry

    lax.fori_loop(1, n, scatter_start, 0)

    def add_and_spread():
        def add(k, value):
            scatter(k)[1].wait_recv()
            return value + landed[k]

        value = lax.fori_loop(1, n, add, own[lax.rem(me, tiles)])
        total[...] = value
        gathered[lax.rem(me, tiles)] = value

        def spread_start(k, carry):
            spread(k).start()
            return carry

        lax.fori_loop(1, n, spread_start, 0)

    if n == tiles:
        add_and_spread()
    else:
        pl.when(me < tiles)(add_and_spread)

    def finish(k, carry):
        owner, copy = scatter(k)
        source = lax.rem(me + n - k, n)
        if n == tiles:
            copy.wait_send()
            spread(k).wait_send()
            spread(k).wait_recv()
        else:
            pl.when(owner < tiles)(lambda: copy.wait_send())
            pl.when(me < tiles)(lambda: spread(k).wait_send())
            pl.when(source < tiles)(lambda: spread(k).wait_recv())
        return carry

    lax.fori_loop(1, n, finish, 0)


def thirds(x):
    high = x.astype(jnp.bfloat16)
    rest = x - high.astype(jnp.float32)
    middle = rest.astype(jnp.bfloat16)
    low = (rest - middle.astype(jnp.float32)).astype(jnp.bfloat16)
    return jnp.concatenate([high, middle, low], axis=0)


def fold(x):
    rows = x.shape[0] // 3
    return x[:rows] + (x[rows : 2 * rows] + x[2 * rows :])


def eliminate(grams):
    size = grams[0].shape[0]
    row_of = lax.broadcasted_iota(jnp.int32, (size, size), 0)
    col_of = lax.broadcasted_iota(jnp.int32, (size, size), 1)
    row_index = lax.broadcasted_iota(jnp.int32, (size, 1), 0)
    eye = (row_of == col_of).astype(jnp.float32)
    pairs = [(gram, eye) for gram in grams]
    for j in range(size):
        done = []
        for left, inverse in pairs:
            scale = lax.rsqrt(left[j : j + 1, j : j + 1])
            left_row = left[j : j + 1] * scale
            inverse_row = inverse[j : j + 1] * scale
            below = jnp.where(row_index > j, left[:, j : j + 1] * scale, 0.0)
            left = jnp.where(row_of == j, left_row, left - below * left_row)
            inverse = jnp.where(row_of == j, inverse_row, inverse - below * inverse_row)
            done.append((left, inverse))
        pairs = done
    return [(jnp.where(col_of >= row_of, left, 0.0), inverse) for left, inverse in pairs]


def times(a, b):
    return jnp.dot(a, b, precision=precise, preferred_element_type=jnp.float32)


def contracted(a, b, axes, precision=None):
    return lax.dot_general(
        a, b, ((axes, axes), ((), ())), precision=precision, preferred_element_type=jnp.float32
    )


def inner(a, b):
    rows = b.shape[0] // 3
    blocks = fold(contracted(a, b, (1,)))
    return blocks[:, :rows] + (blocks[:, rows : 2 * rows] + blocks[:, 2 * rows :])


def iterate_kernel(
    cols,
    x_hbm,
    start_ref,
    field_ref,
    phi_ref,
    x_raw,
    x_ref,
    acc_ref,
    mine,
    theirs,
    blocks,
    edge_row,
    edge_col,
    below_ref,
    beside_ref,
    own,
    landed,
    total,
    gathered,
    load_sem,
    send_p,
    recv_p,
    send_h,
    recv_h,
    send_a,
    recv_a,
    send_b,
    recv_b,
):
    count, sensors = start_ref.shape
    snaps = x_ref.shape[1] // 2
    chunk = mine.shape[2]
    chunks = sensors // chunk
    width = blocks.shape[2]
    parts = sensors // width
    n = device_count()
    mirror = device_of(n - 1 - position())
    upper = lax.axis_index("gx") < lax.axis_size("gx") // 2
    tile_rows, tile_cols = TILE
    across = 2 * snaps // tile_cols

    turn_row = lax.broadcasted_iota(jnp.int32, (width, width), 0)
    turn_col = lax.broadcasted_iota(jnp.int32, (width, width), 1)
    turn = (jnp.where(upper, turn_row, width - 1 - turn_row) == turn_col).astype(jnp.bfloat16)

    def part_of(b):
        return jnp.where(upper, b, parts - 1 - b)

    def turned(values):
        return fold(jnp.dot(thirds(values), turn, preferred_element_type=jnp.float32))

    load = pltpu.make_async_copy(x_hbm, x_raw, load_sem.at[0])
    load.start()
    enter()

    def exchange(c, first_row, here_row, rows):
        return pltpu.make_async_remote_copy(
            src_ref=mine.at[c, pl.ds(first_row, rows)],
            dst_ref=theirs.at[c, pl.ds(here_row, rows)],
            send_sem=send_p.at[c],
            recv_sem=recv_p.at[c],
            device_id=mirror,
            device_id_type=MESH,
        )

    per_chunk = chunk // width
    for c in range(chunks):
        for k in range(per_chunk):
            at = pl.multiple_of(part_of(c * per_chunk + k) * width, width)
            mine[c, :count, k * width : (k + 1) * width] = turned(start_ref[:, pl.ds(at, width)])
        exchange(c, 0, 0, count).start()
    load.wait()
    for b in range(parts):
        at = pl.multiple_of(part_of(b) * width, width)
        for h in range(2):
            x_ref[b * width : (b + 1) * width, h * snaps : (h + 1) * snaps] = jnp.dot(
                turn, x_raw[h, pl.ds(at, width), :], preferred_element_type=jnp.float32
            ).astype(jnp.bfloat16)

    def project(weights_of):
        acc = None
        for c in range(chunks):
            term = jnp.dot(
                thirds(weights_of(c)),
                x_ref[c * chunk : (c + 1) * chunk, :],
                preferred_element_type=jnp.float32,
            )
            acc = term if acc is None else acc + term
        both = fold(acc)
        acc_ref[:, :snaps] = both[:count, :snaps] + both[count:, snaps:]
        acc_ref[:, snaps:] = both[count:, :snaps] - both[:count, snaps:]

    def start_weights(c):
        exchange(c, 0, 0, count).wait()
        here = mine[c, :count]
        there = theirs[c, :count]
        return jnp.concatenate(
            [jnp.where(upper, here, there), jnp.where(upper, -there, here)], axis=0
        )

    def weights(c):
        exchange(c, 0, 0, 2 * count).wait()
        here = mine[c]
        there = theirs[c]
        return jnp.concatenate(
            [here[:count] + there[:count], here[count:] - there[count:]], axis=0
        )

    def reduced(values):
        per_row = values.shape[1] // tile_cols
        places = [
            (i, j) for i in range(values.shape[0] // tile_rows) for j in range(per_row)
        ]
        for t, (i, j) in enumerate(places):
            own[t] = values[
                i * tile_rows : (i + 1) * tile_rows, j * tile_cols : (j + 1) * tile_cols
            ]
        all_reduce(own, landed, total, gathered, send_a, recv_a, send_b, recv_b)
        return jnp.concatenate(
            [
                jnp.concatenate([gathered[i * per_row + j] for j in range(per_row)], axis=1)
                for i in range(values.shape[0] // tile_rows)
            ],
            axis=0,
        )

    def next_side():
        side = reduced(acc_ref[...])
        split = thirds(side)
        ((_, inverse),) = eliminate([inner(split, split)])
        return times(inverse, side)

    def grow(side, first_row, here_row, rows):
        side_first = side[:, :snaps]
        side_second = side[:, snaps:]
        stacked = thirds(
            jnp.concatenate(
                [
                    jnp.concatenate([side_first, -side_second], axis=1),
                    jnp.concatenate([side_second, side_first], axis=1),
                ],
                axis=0,
            )
        )
        for c in range(chunks):
            mine[c] = fold(contracted(stacked, x_ref[c * chunk : (c + 1) * chunk, :], (1,)))
            exchange(c, first_row, here_row, rows).start()

    project(start_weights)

    def step(index, carry):
        grow(next_side(), 0, 0, 2 * count)
        project(weights)
        return carry

    lax.fori_loop(0, ITERS - 1, step, 0)

    sent = pl.multiple_of(jnp.where(upper, count, 0), count)
    grow(next_side(), sent, 0, count)
    for c in range(chunks):
        exchange(c, sent, 0, count).wait()
        there = theirs[c, :count]
        here = jnp.where(upper, mine[c, :count] + there, mine[c, count:] - there)
        for k in range(per_chunk):
            blocks[c * per_chunk + k] = here[:, k * width : (k + 1) * width]
    grown = jnp.concatenate([turned(blocks[part_of(b)]) for b in range(parts)], axis=1)

    edge = edge_row.shape[1]
    sensor_of = lax.broadcasted_iota(jnp.int32, (edge_col.shape[1], sensors), 1)
    line_of = lax.broadcasted_iota(jnp.int32, (edge_col.shape[1], sensors), 0)
    take = (sensor_of == line_of * cols).astype(jnp.bfloat16)
    put = (sensor_of == line_of * cols + cols - 1).astype(jnp.bfloat16)
    split = thirds(grown)
    edge_row[...] = grown[:, :edge]
    edge_col[...] = fold(contracted(split, take, (1,)))
    gx, gy = lax.axis_index("gx"), lax.axis_index("gy")
    nx, ny = lax.axis_size("gx"), lax.axis_size("gy")
    halos = [
        pltpu.make_async_remote_copy(
            src_ref=source,
            dst_ref=target,
            send_sem=send_h.at[k],
            recv_sem=recv_h.at[k],
            device_id=where,
            device_id_type=MESH,
        )
        for k, (source, target, where) in enumerate(
            [
                (edge_row, below_ref, (lax.rem(gx + nx - 1, nx), gy)),
                (edge_col, beside_ref, (gx, lax.rem(gy + ny - 1, ny))),
            ]
        )
    ]
    for halo in halos:
        halo.start()
    sums = [inner(split, split)]
    lane = lax.broadcasted_iota(jnp.int32, (count, sensors), 1)
    lane_edge = lax.broadcasted_iota(jnp.int32, (count, edge), 1)
    shifted_row = pltpu.roll(grown, sensors - cols, 1)
    shifted_col = pltpu.roll(grown, sensors - 1, 1)
    for halo in halos:
        halo.wait()
    tail = jnp.where(
        lane_edge < edge - cols,
        shifted_row[:, sensors - edge :],
        pltpu.roll(below_ref[...], (edge - cols) % edge, 1),
    )
    next_row = (
        tail if sensors == edge else jnp.concatenate([shifted_row[:, : sensors - edge], tail], axis=1)
    )
    last_col = lax.rem(lane, cols) == cols - 1
    beside = fold(jnp.dot(thirds(beside_ref[...]), put, preferred_element_type=jnp.float32))
    next_col = jnp.where(last_col, beside, shifted_col)
    drop_row = (lane >= sensors - cols) & (gx == nx - 1)
    drop_col = last_col & (gy == ny - 1)
    for neighbour, drop in ((next_row, drop_row), (next_col, drop_col)):
        plus = thirds(jnp.where(drop, 0.0, neighbour + grown))
        minus = thirds(jnp.where(drop, 0.0, neighbour - grown))
        sums += [inner(plus, plus), inner(plus, minus)]
    spare = -len(sums) * count % tile_cols
    if spare:
        sums.append(jnp.zeros((count, spare), jnp.float32))
    sums = reduced(jnp.concatenate(sums, axis=1))
    gram, row_lhs, row_rhs, col_lhs, col_rhs = [
        sums[:, k * count : (k + 1) * count] for k in range(5)
    ]
    (upper_factor, inverse), (_, row_inverse), (_, col_inverse) = eliminate(
        [gram, row_lhs, col_lhs]
    )
    field_ref[...] = times(inverse, grown)
    for k, (half, right) in enumerate(((row_inverse, row_rhs), (col_inverse, col_rhs))):
        solved = contracted(half, times(half, right), (0,), precise)
        phi_ref[k] = contracted(times(upper_factor, solved), inverse, (1,), precise)


def dma(*shape):
    return pltpu.SemaphoreType.DMA(shape)


def iterated(x, start, cols):
    count, sensors = start.shape
    n = device_count()
    tiles = count * 2 * x.shape[2] // (TILE[0] * TILE[1])
    chunk = min(512, sensors)
    chunks = sensors // chunk
    width = min(256, chunk)
    edge = -(-cols // TILE[1]) * TILE[1]
    lines = -(-(sensors // cols) // TILE[1]) * TILE[1]
    vmem = pl.BlockSpec(memory_space=pltpu.VMEM)

    def held(*shape):
        return pltpu.VMEM(shape, jnp.float32)

    return pl.pallas_call(
        functools.partial(iterate_kernel, cols),
        out_shape=[
            jax.ShapeDtypeStruct(start.shape, jnp.float32),
            jax.ShapeDtypeStruct((2, count, count), jnp.float32),
        ],
        in_specs=[pl.BlockSpec(memory_space=pl.ANY), vmem],
        out_specs=[vmem, vmem],
        scratch_shapes=[
            pltpu.VMEM(x.shape, jnp.bfloat16),
            pltpu.VMEM((sensors, 2 * x.shape[2]), jnp.bfloat16),
            held(count, 2 * x.shape[2]),
            held(chunks, 2 * count, chunk),
            held(chunks, 2 * count, chunk),
            held(sensors // width, count, width),
            held(count, edge),
            held(count, lines),
            held(count, edge),
            held(count, lines),
            held(tiles, *TILE),
            held(n, *TILE),
            held(*TILE),
            held(tiles, *TILE),
            dma(1),
            dma(chunks),
            dma(chunks),
            dma(2),
            dma(2),
            dma(n),
            dma(n),
            dma(n),
            dma(n),
        ],
        compiler_params=pltpu.CompilerParams(
            collective_id=0, has_side_effects=True, vmem_limit_bytes=48 * 2**20
        ),
    )(x, start)


def body(snapshots, start):
    frames, count, rows, cols = start.shape
    snaps = snapshots.shape[-1]
    fields = []
    phis = []
    for frame in range(frames):
        field, phi = iterated(
            snapshots[:, frame].reshape(2, rows * cols, snaps),
            start[frame].reshape(count, rows * cols),
            cols,
        )
        fields.append(field.reshape(count, rows, cols))
        phis.append(phi)
    return (jnp.stack(fields), jnp.stack(phis))


def solution(mesh):
    return jax.shard_map(
        body,
        mesh=mesh,
        in_specs=(P(None, None, "gx", "gy", None), P(None, None, "gx", "gy")),
        out_specs=(P(None, None, "gx", "gy"), P()),
        check_vma=False,
    )
```

```python
import functools

import jax
import jax.numpy as jnp
from jax import lax
from jax.experimental import pallas as pl
from jax.experimental.pallas import tpu as pltpu
from jax.sharding import PartitionSpec as P

ITERS = 4
TILE = (8, 128)
MESH = pl.DeviceIdType.MESH

precise = lax.Precision.HIGHEST


def position():
    across = lax.axis_size("gy")
    return lax.axis_index("gx") * across + lax.axis_index("gy")


def device_of(index):
    across = lax.axis_size("gy")
    return (lax.div(index, across), lax.rem(index, across))


def device_count():
    return lax.axis_size("gx") * lax.axis_size("gy")


def enter():
    n = device_count()
    me = position()
    barrier = pltpu.get_barrier_semaphore()

    def greet(k, carry):
        pl.semaphore_signal(
            barrier, inc=1, device_id=device_of(lax.rem(me + k, n)), device_id_type=MESH
        )
        return carry

    lax.fori_loop(1, n, greet, 0)
    pl.semaphore_wait(barrier, n - 1)


def all_reduce(own, landed, total, gathered, send_a, recv_a, send_b, recv_b):
    n = device_count()
    me = position()
    tiles = own.shape[0]

    def scatter(k):
        owner = lax.rem(me + k, n)
        return owner, pltpu.make_async_remote_copy(
            src_ref=own.at[lax.rem(owner, tiles)],
            dst_ref=landed.at[k],
            send_sem=send_a.at[k],
            recv_sem=recv_a.at[k],
            device_id=device_of(owner),
            device_id_type=MESH,
        )

    def spread(k):
        return pltpu.make_async_remote_copy(
            src_ref=total,
            dst_ref=gathered.at[lax.rem(me, tiles)],
            send_sem=send_b.at[k],
            recv_sem=recv_b.at[k],
            device_id=device_of(lax.rem(me + k, n)),
            device_id_type=MESH,
        )

    def scatter_start(k, carry):
        owner, copy = scatter(k)
        if n == tiles:
            copy.start()
        else:
            pl.when(owner < tiles)(lambda: copy.start())
        return carry

    lax.fori_loop(1, n, scatter_start, 0, unroll=n <= 32)

    def add_and_spread():
        def add(k, value):
            scatter(k)[1].wait_recv()
            return value + landed[k]

        value = lax.fori_loop(1, n, add, own[lax.rem(me, tiles)], unroll=n <= 32)
        total[...] = value
        gathered[lax.rem(me, tiles)] = value

        def spread_start(k, carry):
            spread(k).start()
            return carry

        lax.fori_loop(1, n, spread_start, 0, unroll=n <= 32)

    if n == tiles:
        add_and_spread()
    else:
        pl.when(me < tiles)(add_and_spread)

    def finish(k, carry):
        owner, copy = scatter(k)
        source = lax.rem(me + n - k, n)
        if n == tiles:
            copy.wait_send()
            spread(k).wait_send()
            spread(k).wait_recv()
        else:
            pl.when(owner < tiles)(lambda: copy.wait_send())
            pl.when(me < tiles)(lambda: spread(k).wait_send())
            pl.when(source < tiles)(lambda: spread(k).wait_recv())
        return carry

    lax.fori_loop(1, n, finish, 0)


def thirds(x):
    high = x.astype(jnp.bfloat16)
    rest = x - high.astype(jnp.float32)
    middle = rest.astype(jnp.bfloat16)
    low = (rest - middle.astype(jnp.float32)).astype(jnp.bfloat16)
    return jnp.concatenate([high, middle, low], axis=0)


def fold(x):
    rows = x.shape[0] // 3
    return x[:rows] + (x[rows : 2 * rows] + x[2 * rows :])


def eliminate(grams):
    size = grams[0].shape[0]
    row_of = lax.broadcasted_iota(jnp.int32, (size, size), 0)
    col_of = lax.broadcasted_iota(jnp.int32, (size, size), 1)
    row_index = lax.broadcasted_iota(jnp.int32, (size, 1), 0)
    eye = (row_of == col_of).astype(jnp.float32)
    pairs = [(gram, eye) for gram in grams]
    for j in range(size):
        done = []
        for left, inverse in pairs:
            scale = lax.rsqrt(left[j : j + 1, j : j + 1])
            left_row = left[j : j + 1] * scale
            inverse_row = inverse[j : j + 1] * scale
            below = jnp.where(row_index > j, left[:, j : j + 1] * scale, 0.0)
            left = jnp.where(row_of == j, left_row, left - below * left_row)
            inverse = jnp.where(row_of == j, inverse_row, inverse - below * inverse_row)
            done.append((left, inverse))
        pairs = done
    return [(jnp.where(col_of >= row_of, left, 0.0), inverse) for left, inverse in pairs]


def times(a, b):
    return jnp.dot(a, b, precision=precise, preferred_element_type=jnp.float32)


def contracted(a, b, axes, precision=None):
    return lax.dot_general(
        a, b, ((axes, axes), ((), ())), precision=precision, preferred_element_type=jnp.float32
    )


def inner(a, b):
    rows = b.shape[0] // 3
    blocks = fold(contracted(a, b, (1,)))
    return blocks[:, :rows] + (blocks[:, rows : 2 * rows] + blocks[:, 2 * rows :])


def iterate_kernel(
    cols,
    x_hbm,
    start_ref,
    field_ref,
    phi_ref,
    x_raw,
    x_ref,
    acc_ref,
    mine,
    theirs,
    blocks,
    edge_row,
    edge_col,
    below_ref,
    beside_ref,
    own,
    landed,
    total,
    gathered,
    load_sem,
    send_p,
    recv_p,
    send_h,
    recv_h,
    send_a,
    recv_a,
    send_b,
    recv_b,
):
    count, sensors = start_ref.shape
    snaps = x_ref.shape[1] // 2
    chunk = mine.shape[2]
    chunks = sensors // chunk
    width = blocks.shape[2]
    parts = sensors // width
    n = device_count()
    mirror = device_of(n - 1 - position())
    upper = lax.axis_index("gx") < lax.axis_size("gx") // 2
    tile_rows, tile_cols = TILE
    across = 2 * snaps // tile_cols

    turn_row = lax.broadcasted_iota(jnp.int32, (width, width), 0)
    turn_col = lax.broadcasted_iota(jnp.int32, (width, width), 1)
    turn = (jnp.where(upper, turn_row, width - 1 - turn_row) == turn_col).astype(jnp.bfloat16)

    def part_of(b):
        return jnp.where(upper, b, parts - 1 - b)

    def turned(values):
        return fold(jnp.dot(thirds(values), turn, preferred_element_type=jnp.float32))

    load = pltpu.make_async_copy(x_hbm, x_raw, load_sem.at[0])
    load.start()
    enter()

    def exchange(c, first_row, here_row, rows):
        return pltpu.make_async_remote_copy(
            src_ref=mine.at[c, pl.ds(first_row, rows)],
            dst_ref=theirs.at[c, pl.ds(here_row, rows)],
            send_sem=send_p.at[c],
            recv_sem=recv_p.at[c],
            device_id=mirror,
            device_id_type=MESH,
        )

    per_chunk = chunk // width
    for c in range(chunks):
        for k in range(per_chunk):
            at = pl.multiple_of(part_of(c * per_chunk + k) * width, width)
            mine[c, :count, k * width : (k + 1) * width] = turned(start_ref[:, pl.ds(at, width)])
        exchange(c, 0, 0, count).start()
    load.wait()
    for b in range(parts):
        at = pl.multiple_of(part_of(b) * width, width)
        for h in range(2):
            x_ref[b * width : (b + 1) * width, h * snaps : (h + 1) * snaps] = jnp.dot(
                turn, x_raw[h, pl.ds(at, width), :], preferred_element_type=jnp.float32
            ).astype(jnp.bfloat16)

    def project(weights_of):
        acc = None
        for c in range(chunks):
            term = jnp.dot(
                thirds(weights_of(c)),
                x_ref[c * chunk : (c + 1) * chunk, :],
                preferred_element_type=jnp.float32,
            )
            acc = term if acc is None else acc + term
        both = fold(acc)
        acc_ref[:, :snaps] = both[:count, :snaps] + both[count:, snaps:]
        acc_ref[:, snaps:] = both[count:, :snaps] - both[:count, snaps:]

    def start_weights(c):
        exchange(c, 0, 0, count).wait()
        here = mine[c, :count]
        there = theirs[c, :count]
        return jnp.concatenate(
            [jnp.where(upper, here, there), jnp.where(upper, -there, here)], axis=0
        )

    def weights(c):
        exchange(c, 0, 0, 2 * count).wait()
        here = mine[c]
        there = theirs[c]
        return jnp.concatenate(
            [here[:count] + there[:count], here[count:] - there[count:]], axis=0
        )

    def reduced(values):
        per_row = values.shape[1] // tile_cols
        places = [
            (i, j) for i in range(values.shape[0] // tile_rows) for j in range(per_row)
        ]
        for t, (i, j) in enumerate(places):
            own[t] = values[
                i * tile_rows : (i + 1) * tile_rows, j * tile_cols : (j + 1) * tile_cols
            ]
        all_reduce(own, landed, total, gathered, send_a, recv_a, send_b, recv_b)
        return jnp.concatenate(
            [
                jnp.concatenate([gathered[i * per_row + j] for j in range(per_row)], axis=1)
                for i in range(values.shape[0] // tile_rows)
            ],
            axis=0,
        )

    def next_side():
        side = reduced(acc_ref[...])
        split = thirds(side)
        ((_, inverse),) = eliminate([inner(split, split)])
        return times(inverse, side)

    def grow(side, first_row, here_row, rows):
        side_first = side[:, :snaps]
        side_second = side[:, snaps:]
        stacked = thirds(
            jnp.concatenate(
                [
                    jnp.concatenate([side_first, -side_second], axis=1),
                    jnp.concatenate([side_second, side_first], axis=1),
                ],
                axis=0,
            )
        )
        for c in range(chunks):
            mine[c] = fold(contracted(stacked, x_ref[c * chunk : (c + 1) * chunk, :], (1,)))
            exchange(c, first_row, here_row, rows).start()

    project(start_weights)

    def step(index, carry):
        grow(next_side(), 0, 0, 2 * count)
        project(weights)
        return carry

    lax.fori_loop(0, ITERS - 1, step, 0)

    sent = pl.multiple_of(jnp.where(upper, count, 0), count)
    grow(next_side(), sent, 0, count)
    for c in range(chunks):
        exchange(c, sent, 0, count).wait()
        there = theirs[c, :count]
        here = jnp.where(upper, mine[c, :count] + there, mine[c, count:] - there)
        for k in range(per_chunk):
            blocks[c * per_chunk + k] = here[:, k * width : (k + 1) * width]
    grown = jnp.concatenate([turned(blocks[part_of(b)]) for b in range(parts)], axis=1)

    edge = edge_row.shape[1]
    sensor_of = lax.broadcasted_iota(jnp.int32, (edge_col.shape[1], sensors), 1)
    line_of = lax.broadcasted_iota(jnp.int32, (edge_col.shape[1], sensors), 0)
    take = (sensor_of == line_of * cols).astype(jnp.bfloat16)
    put = (sensor_of == line_of * cols + cols - 1).astype(jnp.bfloat16)
    split = thirds(grown)
    edge_row[...] = grown[:, :edge]
    edge_col[...] = fold(contracted(split, take, (1,)))
    gx, gy = lax.axis_index("gx"), lax.axis_index("gy")
    nx, ny = lax.axis_size("gx"), lax.axis_size("gy")
    halos = [
        pltpu.make_async_remote_copy(
            src_ref=source,
            dst_ref=target,
            send_sem=send_h.at[k],
            recv_sem=recv_h.at[k],
            device_id=where,
            device_id_type=MESH,
        )
        for k, (source, target, where) in enumerate(
            [
                (edge_row, below_ref, (lax.rem(gx + nx - 1, nx), gy)),
                (edge_col, beside_ref, (gx, lax.rem(gy + ny - 1, ny))),
            ]
        )
    ]
    for halo in halos:
        halo.start()
    sums = [inner(split, split)]
    lane = lax.broadcasted_iota(jnp.int32, (count, sensors), 1)
    lane_edge = lax.broadcasted_iota(jnp.int32, (count, edge), 1)
    shifted_row = pltpu.roll(grown, sensors - cols, 1)
    shifted_col = pltpu.roll(grown, sensors - 1, 1)
    for halo in halos:
        halo.wait()
    tail = jnp.where(
        lane_edge < edge - cols,
        shifted_row[:, sensors - edge :],
        pltpu.roll(below_ref[...], (edge - cols) % edge, 1),
    )
    next_row = (
        tail if sensors == edge else jnp.concatenate([shifted_row[:, : sensors - edge], tail], axis=1)
    )
    last_col = lax.rem(lane, cols) == cols - 1
    beside = fold(jnp.dot(thirds(beside_ref[...]), put, preferred_element_type=jnp.float32))
    next_col = jnp.where(last_col, beside, shifted_col)
    drop_row = (lane >= sensors - cols) & (gx == nx - 1)
    drop_col = last_col & (gy == ny - 1)
    for neighbour, drop in ((next_row, drop_row), (next_col, drop_col)):
        plus = thirds(jnp.where(drop, 0.0, neighbour + grown))
        minus = thirds(jnp.where(drop, 0.0, neighbour - grown))
        sums += [inner(plus, plus), inner(plus, minus)]
    spare = -len(sums) * count % tile_cols
    if spare:
        sums.append(jnp.zeros((count, spare), jnp.float32))
    sums = reduced(jnp.concatenate(sums, axis=1))
    gram, row_lhs, row_rhs, col_lhs, col_rhs = [
        sums[:, k * count : (k + 1) * count] for k in range(5)
    ]
    (upper_factor, inverse), (_, row_inverse), (_, col_inverse) = eliminate(
        [gram, row_lhs, col_lhs]
    )
    field_ref[...] = times(inverse, grown)
    for k, (half, right) in enumerate(((row_inverse, row_rhs), (col_inverse, col_rhs))):
        solved = contracted(half, times(half, right), (0,), precise)
        phi_ref[k] = contracted(times(upper_factor, solved), inverse, (1,), precise)


def dma(*shape):
    return pltpu.SemaphoreType.DMA(shape)


def iterated(x, start, cols):
    count, sensors = start.shape
    n = device_count()
    tiles = count * 2 * x.shape[2] // (TILE[0] * TILE[1])
    chunk = min(512, sensors)
    chunks = sensors // chunk
    width = min(256, chunk)
    edge = -(-cols // TILE[1]) * TILE[1]
    lines = -(-(sensors // cols) // TILE[1]) * TILE[1]
    vmem = pl.BlockSpec(memory_space=pltpu.VMEM)

    def held(*shape):
        return pltpu.VMEM(shape, jnp.float32)

    return pl.pallas_call(
        functools.partial(iterate_kernel, cols),
        out_shape=[
            jax.ShapeDtypeStruct(start.shape, jnp.float32),
            jax.ShapeDtypeStruct((2, count, count), jnp.float32),
        ],
        in_specs=[pl.BlockSpec(memory_space=pl.ANY), vmem],
        out_specs=[vmem, vmem],
        scratch_shapes=[
            pltpu.VMEM(x.shape, jnp.bfloat16),
            pltpu.VMEM((sensors, 2 * x.shape[2]), jnp.bfloat16),
            held(count, 2 * x.shape[2]),
            held(chunks, 2 * count, chunk),
            held(chunks, 2 * count, chunk),
            held(sensors // width, count, width),
            held(count, edge),
            held(count, lines),
            held(count, edge),
            held(count, lines),
            held(tiles, *TILE),
            held(n, *TILE),
            held(*TILE),
            held(tiles, *TILE),
            dma(1),
            dma(chunks),
            dma(chunks),
            dma(2),
            dma(2),
            dma(n),
            dma(n),
            dma(n),
            dma(n),
        ],
        compiler_params=pltpu.CompilerParams(
            collective_id=0, has_side_effects=True, vmem_limit_bytes=48 * 2**20
        ),
    )(x, start)


def body(snapshots, start):
    frames, count, rows, cols = start.shape
    snaps = snapshots.shape[-1]
    fields = []
    phis = []
    for frame in range(frames):
        field, phi = iterated(
            snapshots[:, frame].reshape(2, rows * cols, snaps),
            start[frame].reshape(count, rows * cols),
            cols,
        )
        fields.append(field.reshape(count, rows, cols))
        phis.append(phi)
    return (jnp.stack(fields), jnp.stack(phis))


def solution(mesh):
    return jax.shard_map(
        body,
        mesh=mesh,
        in_specs=(P(None, None, "gx", "gy", None), P(None, None, "gx", "gy")),
        out_specs=(P(None, None, "gx", "gy"), P()),
        check_vma=False,
    )
```
